32 devices in a mesh: expert: 4 (over y, x), shard: 8 (over z, core).
Axes of the slice: x: 2, y: 2, z: 4, core: 2. Of those that a mesh axis runs over, the one named last changes fastest.
Arguments:
- master_gate: float32 [128, 2048, 768], P('expert', 'shard'), may hold values from -0.1875 to 0.1875
- master_up: float32 [128, 2048, 768], P('expert', 'shard'), may hold values from -0.1875 to 0.1875
- router_weight: float32 [2048, 128], P('shard', 'expert'), may hold values from -0.125 to 0.125
- router_gain: float32 [2048], P('shard'), may hold values from 0.25 to 1.75
Outputs:
- final_gate: bfloat16 [128, 2048, 768], P(('expert', 'shard'))
- final_up: bfloat16 [128, 2048, 768], P(('expert', 'shard'))
- scale_gate: float32 [128, 768], P(('expert', 'shard'))
- scale_up: float32 [128, 768], P(('expert', 'shard'))
- serve_router: bfloat16 [2048, 128], replicated
The draws below stay inside these ranges and needn't reach their ends.
All inputs are finite; a program needn't handle non-finite values. Where the reference program divides by a largest or mean magnitude, that divisor is 1e-20 or more.
Results may differ from the reference program's by a relative error of at most 0.001.
Values may be sent and summed in bfloat16 or wider, within the bound.
A program may use at most 192 MiB of HBM per device.

```python
import jax
import jax.numpy as jnp

EXPERTS = 128
D_MODEL = 2048
D_EXPERT = 768


def spiked(array, key, source, target, parts, factor):
    def block_of(dim):
        return (jnp.arange(array.shape[dim]) // (array.shape[dim] // parts)).reshape((-1,) + (1,) * (array.ndim - 1 - dim))

    one_side = jax.random.permutation(key, parts)[block_of(target)]
    other_side = (block_of(target) + parts // 2) % parts
    return jnp.where((block_of(source) == one_side) | (block_of(source) == other_side), factor * array, array)


def shard_levels(own_key, extent, split, low, largest):
    loudness, own = 1.0, jax.random.fold_in(own_key, 6)
    for position, shards_of in split:
        heights = jnp.exp(jax.random.uniform(jax.random.fold_in(own, position), (shards_of,), jnp.float32, low / len(split), largest / len(split)))
        loudness = loudness * jnp.repeat(heights, extent[position] // shards_of).reshape([-1 if axis == position else 1 for axis in range(len(extent))])
    return loudness


def gaussian(rng, shape, spread, most, cuts=(), held_as=jnp.bfloat16):
    gain = shard_levels(rng, shape, cuts, -0.22, 0.18) if cuts else 1.0
    array = jax.random.normal(rng, shape, jnp.float32) * spread * gain
    return jnp.minimum(jnp.maximum(array, -most), most).astype(held_as)


def gaussian_with(own_key, dims, deviation, bound, cuts, heavy, kind=jnp.bfloat16):
    array = deviation * jax.random.normal(own_key, dims, jnp.float32)
    if cuts:
        array = array * shard_levels(own_key, dims, cuts, -0.22, 0.18)
    return jnp.clip(spiked(array, jax.random.fold_in(own_key, 3), *heavy), -bound, bound).astype(kind)


def setup_inputs(seed: int = 0) -> dict:
    streams_of = jax.random.split(jax.random.key(seed), 5)
    return {
        "master_gate": gaussian_with(streams_of[0], (EXPERTS, D_MODEL, D_EXPERT), D_MODEL ** -0.5, 0.1875, ((0, 4), (1, 8)), (1, 2, 8, 2.0), jnp.float32),
        "master_up": gaussian_with(streams_of[1], (EXPERTS, D_MODEL, D_EXPERT), D_MODEL ** -0.5, 0.1875, ((0, 4), (1, 8)), (1, 2, 8, 2.0), jnp.float32),
        "router_weight": gaussian(streams_of[2], (D_MODEL, EXPERTS), D_MODEL ** -0.5, 0.125, ((0, 8), (1, 4)), jnp.float32),
        "router_gain": jnp.clip(1.0 + 0.15 * jax.random.normal(streams_of[3], (D_MODEL,), jnp.float32), 0.25, 1.75),
    }


def reference(master_gate, master_up, router_weight, router_gain):
    scale_gate = jnp.sum(jnp.abs(master_gate), axis=1) / D_MODEL
    final_gate = (master_gate / jnp.expand_dims(scale_gate, 1)).astype(jnp.bfloat16)
    scale_up = jnp.sum(jnp.abs(master_up), axis=1) / D_MODEL
    final_up = (master_up / jnp.expand_dims(scale_up, 1)).astype(jnp.bfloat16)
    serve_router = (router_weight * router_gain[:, None]).astype(jnp.bfloat16)
    return final_gate, final_up, scale_gate, scale_up, serve_router
```

```python
import functools

import jax
import jax.numpy as jnp
from jax import lax
from jax.experimental import pallas as pl
from jax.experimental.pallas import tpu as pltpu
from jax.sharding import PartitionSpec as P

MESH = pl.DeviceIdType.MESH
SLOTS = 4
LEAD = 4


def sum_order(n):
    chips = n // 2
    return sorted(range(n), key=lambda g: (abs(2 * (g // 2) - (chips - 1)), g % 2, g))


def send_order(n, me):
    chip = me // 2
    order = sum_order(n)
    others = [g for g in range(n) if g // 2 != chip]
    return sorted(others, key=lambda g: (abs(g // 2 - chip), g % 2, order.index(g)))


def pick(me, values):
    result = jnp.int32(values[0])
    for i in range(1, len(values)):
        result = jnp.where(me == i, jnp.int32(values[i]), result)
    return result


def kernel(
    n, ne, rows_total,
    gate, up, router_t, gain,
    final_gate, final_up, scale_gate, scale_up, out_router_t,
    ring, sbuf, psum, parts, scales, routers,
    read_sem, psum_send, psum_recv, scale_send, scale_recv,
    data_send, data_recv, row_send, row_recv, col_send, col_recv,
):
    me = lax.axis_index("shard")
    mine = lax.axis_index("expert")
    per = final_gate.shape[0]
    rows, cols = gate.shape[1], gate.shape[2]
    sources, finals = (gate, up), (final_gate, final_up)

    order = sum_order(n)
    tables = [send_order(n, i) for i in range(n)]
    remote = [pick(me, [tables[i][k] for i in range(n)]) for k in range(n - 2)]
    partner = me + 1 - 2 * lax.rem(me, 2)
    targets = [remote[0], partner, me] + remote[1:]

    work = []
    for i in range(LEAD):
        work += [("sum", i, order[i], t) for t in (0, 1)]
    work += [("send", 0, targets[0], t) for t in (0, 1)]
    for i in range(LEAD, n):
        work += [("sum", i, order[i], t) for t in (0, 1)]
    for k in range(1, n):
        work += [("send", k, targets[k], t) for t in (0, 1)]

    def read(index):
        _, _, group, t = work[index]
        slot = index % SLOTS
        return pltpu.make_async_copy(
            sources[t].at[pl.ds(group * per, per)], ring.at[slot], read_sem.at[slot]
        )

    for index in range(SLOTS):
        read(index).start()

    def peer(j):
        return lax.rem(me + j, n)

    def other(j):
        return lax.rem(mine + j, ne)

    def psum_copy(group):
        return pltpu.make_async_remote_copy(
            src_ref=psum.at[group], dst_ref=parts.at[me], send_sem=psum_send.at[group],
            recv_sem=psum_recv.at[me], device_id={"shard": group}, device_id_type=MESH,
        )

    def psum_arrival(source):
        return pltpu.make_async_remote_copy(
            src_ref=parts.at[source], dst_ref=parts.at[source], send_sem=psum_send.at[source],
            recv_sem=psum_recv.at[source], device_id={"shard": source}, device_id_type=MESH,
        )

    def scale_copy(j):
        return pltpu.make_async_remote_copy(
            src_ref=scales.at[me], dst_ref=scales.at[me], send_sem=scale_send.at[j],
            recv_sem=scale_recv.at[me], device_id={"shard": peer(j)}, device_id_type=MESH,
        )

    def scale_arrival(group):
        return pltpu.make_async_remote_copy(
            src_ref=scales.at[group], dst_ref=scales.at[group], send_sem=scale_send.at[0],
            recv_sem=scale_recv.at[group], device_id={"shard": group}, device_id_type=MESH,
        )

    def data_copy(k, t, e):
        return pltpu.make_async_remote_copy(
            src_ref=sbuf.at[k, t * per + e],
            dst_ref=finals[t].at[e, pl.ds(me * rows, rows)],
            send_sem=data_send.at[k, t * per + e],
            recv_sem=data_recv.at[me, t * per + e],
            device_id={"shard": targets[k]}, device_id_type=MESH,
        )

    def own_copy(k, t, e):
        return pltpu.make_async_copy(
            sbuf.at[k, t * per + e],
            finals[t].at[e, pl.ds(me * rows, rows)],
            data_send.at[k, t * per + e],
        )

    def data_arrival(source, t, e):
        return pltpu.make_async_remote_copy(
            src_ref=finals[t].at[e, pl.ds(source * rows, rows)],
            dst_ref=finals[t].at[e, pl.ds(source * rows, rows)],
            send_sem=data_send.at[0, t * per + e],
            recv_sem=data_recv.at[source, t * per + e],
            device_id={"shard": source}, device_id_type=MESH,
        )

    def row_copy(j):
        return pltpu.make_async_remote_copy(
            src_ref=routers.at[mine, me], dst_ref=routers.at[mine, me], send_sem=row_send.at[j],
            recv_sem=row_recv.at[me], device_id={"shard": peer(j)}, device_id_type=MESH,
        )

    def row_arrival(source):
        return pltpu.make_async_remote_copy(
            src_ref=routers.at[mine, source], dst_ref=routers.at[mine, source],
            send_sem=row_send.at[0], recv_sem=row_recv.at[source],
            device_id={"shard": source}, device_id_type=MESH,
        )

    def col_copy(j):
        return pltpu.make_async_remote_copy(
            src_ref=routers.at[mine], dst_ref=routers.at[mine], send_sem=col_send.at[j],
            recv_sem=col_recv.at[mine], device_id={"expert": other(j)}, device_id_type=MESH,
        )

    def col_arrival(source):
        return pltpu.make_async_remote_copy(
            src_ref=routers.at[source], dst_ref=routers.at[source], send_sem=col_send.at[0],
            recv_sem=col_recv.at[source], device_id={"expert": source}, device_id_type=MESH,
        )

    barrier = pltpu.get_barrier_semaphore()
    for j in range(1, n):
        pl.semaphore_signal(barrier, inc=1, device_id={"shard": peer(j)}, device_id_type=MESH)
    for j in range(1, ne):
        pl.semaphore_signal(barrier, inc=1, device_id={"expert": other(j)}, device_id_type=MESH)

    def sum_chunk(slot, group, t):
        def one(e, _):
            def block(b, total):
                start = pl.multiple_of(b * 8, 8)
                return total + jnp.abs(ring[slot, e, pl.ds(start, 8), :])

            total = lax.fori_loop(
                0, rows // 8, block, jnp.zeros((8, cols), jnp.float32), unroll=8
            )
            psum[group, pl.ds(t * per + e, 1), :] = jnp.sum(total, axis=0, keepdims=True)
            return 0

        lax.fori_loop(0, per, one, 0)

    def send_chunk(slot, k, group, t):
        def one(e, _):
            inverse = 1.0 / scales[group, pl.ds(t * per + e, 1), :]
            wide = jnp.broadcast_to(inverse, (16, cols))

            def block(b, _):
                start = pl.multiple_of(b * 16, 16)
                sbuf[k, t * per + e, pl.ds(start, 16), :] = (
                    ring[slot, e, pl.ds(start, 16), :] * wide
                ).astype(jnp.bfloat16)
                return 0

            lax.fori_loop(0, rows // 16, block, 0, unroll=4)
            if k == 2:
                own_copy(k, t, e).start()
            else:
                data_copy(k, t, e).start()
            return 0

        lax.fori_loop(0, per, one, 0)

    def home():
        for j in range(1, n):
            psum_arrival(peer(j)).wait_recv()
        parts[me] = psum[me]
        total = parts[0]
        for i in range(1, n):
            total = total + parts[i]
        scale = total / rows_total
        scales[me] = scale
        for j in range(1, n):
            scale_copy(j).start()
        scale_gate[...] = scale[:per]
        scale_up[...] = scale[per:]

    early = me == order[0]
    for i in range(1, LEAD // 2):
        early = jnp.logical_or(early, me == order[i])

    for index, (kind, step, group, t) in enumerate(work):
        slot = index % SLOTS
        if kind == "send" and t == 0:
            if step == 0:
                pl.when(early)(home)
            elif step == 1:
                pl.when(jnp.logical_not(early))(home)
                routers[mine, me] = (router_t[...] * gain[...]).astype(jnp.bfloat16)
                for j in range(1, n):
                    row_copy(j).start()
            if step != 2:
                scale_arrival(group).wait_recv()
        read(index).wait()
        if kind == "sum":
            sum_chunk(slot, group, t)
            if t == 1:
                if step == 0:
                    pl.semaphore_wait(barrier, n - 1 + ne - 1)

                @pl.when(me != group)
                def _(group=group):
                    psum_copy(group).start()
        else:
            send_chunk(slot, step, group, t)
        if index + SLOTS < len(work):
            read(index + SLOTS).start()

    for j in range(1, n):
        row_arrival(peer(j)).wait_recv()
    for j in range(1, ne):
        col_copy(j).start()
    for j in range(1, ne):
        col_arrival(other(j)).wait_recv()
    wide, tall = routers.shape[2], routers.shape[3]
    for e in range(ne):
        for s in range(n):
            out_router_t[e * wide:(e + 1) * wide, s * tall:(s + 1) * tall] = routers[e, s]

    for j in range(1, n):
        psum_copy(peer(j)).wait_send()
        scale_copy(j).wait_send()
        row_copy(j).wait_send()
    for j in range(1, ne):
        col_copy(j).wait_send()
    for k in range(n):
        for t in (0, 1):

            def done(e, _, k=k, t=t):
                if k == 2:
                    own_copy(k, t, e).wait()
                else:
                    data_copy(k, t, e).wait_send()
                return 0

            lax.fori_loop(0, per, done, 0)
    for j in range(1, n):
        for t in (0, 1):

            def arrived(e, _, j=j, t=t):
                data_arrival(peer(j), t, e).wait_recv()
                return 0

            lax.fori_loop(0, per, arrived, 0)


def solution(mesh):
    n, ne = mesh.shape["shard"], mesh.shape["expert"]

    def body(master_gate, master_up, router_weight, router_gain):
        held, rows, cols = master_gate.shape
        per = held // n
        router_t = router_weight.T
        wide, tall = router_t.shape
        sem = pltpu.SemaphoreType.DMA
        final_gate, final_up, scale_gate, scale_up, serve_t = pl.pallas_call(
            functools.partial(kernel, n, ne, rows * n),
            out_shape=(
                jax.ShapeDtypeStruct((per, rows * n, cols), jnp.bfloat16),
                jax.ShapeDtypeStruct((per, rows * n, cols), jnp.bfloat16),
                jax.ShapeDtypeStruct((per, cols), jnp.float32),
                jax.ShapeDtypeStruct((per, cols), jnp.float32),
                jax.ShapeDtypeStruct((wide * ne, tall * n), jnp.bfloat16),
            ),
            in_specs=[
                pl.BlockSpec(memory_space=pl.ANY),
                pl.BlockSpec(memory_space=pl.ANY),
                pl.BlockSpec(memory_space=pltpu.VMEM),
                pl.BlockSpec(memory_space=pltpu.VMEM),
            ],
            out_specs=(
                pl.BlockSpec(memory_space=pl.ANY),
                pl.BlockSpec(memory_space=pl.ANY),
                pl.BlockSpec(memory_space=pltpu.VMEM),
                pl.BlockSpec(memory_space=pltpu.VMEM),
                pl.BlockSpec(memory_space=pltpu.VMEM),
            ),
            scratch_shapes=[
                pltpu.VMEM((SLOTS, per, rows, cols), jnp.float32),
                pltpu.VMEM((n, 2 * per, rows, cols), jnp.bfloat16),
                pltpu.VMEM((n, 2 * per, cols), jnp.float32),
                pltpu.VMEM((n, 2 * per, cols), jnp.float32),
                pltpu.VMEM((n, 2 * per, cols), jnp.float32),
                pltpu.VMEM((ne, n, wide, tall), jnp.bfloat16),
                sem((SLOTS,)),
                sem((n,)), sem((n,)), sem((n,)), sem((n,)),
                sem((n, 2 * per)), sem((n, 2 * per)),
                sem((n,)), sem((n,)), sem((ne,)), sem((ne,)),
            ],
            compiler_params=pltpu.CompilerParams(
                collective_id=0, has_side_effects=True, vmem_limit_bytes=60 * 1024 * 1024
            ),
        )(master_gate, master_up, router_t, router_gain[None, :])
        return final_gate, final_up, scale_gate, scale_up, serve_t.T

    return jax.shard_map(
        body,
        mesh=mesh,
        in_specs=(
            P("expert", "shard", None),
            P("expert", "shard", None),
            P("shard", "expert"),
            P("shard"),
        ),
        out_specs=(
            P(("expert", "shard"), None, None),
            P(("expert", "shard"), None, None),
            P(("expert", "shard"), None),
            P(("expert", "shard"), None),
            P(),
        ),
        check_vma=False,
    )
```

```python
import functools

import jax
import jax.numpy as jnp
from jax import lax
from jax.experimental import pallas as pl
from jax.experimental.pallas import tpu as pltpu
from jax.sharding import PartitionSpec as P

MESH = pl.DeviceIdType.MESH
SLOTS = 4
LEAD = 4
VMEM_BYTES = 38 * 1024 * 1024


def sum_order(n):
    chips = n // 2
    return sorted(range(n), key=lambda g: (abs(2 * (g // 2) - (chips - 1)), g % 2, g))


def send_order(n, me):
    chip = me // 2
    order = sum_order(n)
    others = [g for g in range(n) if g // 2 != chip]
    return sorted(others, key=lambda g: (abs(g // 2 - chip), g % 2, order.index(g)))


def pick(me, values):
    result = jnp.int32(values[0])
    for i in range(1, len(values)):
        result = jnp.where(me == i, jnp.int32(values[i]), result)
    return result


def kernel(
    n, ne, rows_total,
    gate, up, router_t, gain,
    final_gate, final_up, scale_gate, scale_up, out_router_t,
    ring, sbuf, psum, parts, scales, routers,
    read_sem, psum_send, psum_recv, scale_send, scale_recv,
    data_send, data_recv, row_send, row_recv, col_send, col_recv,
):
    me = lax.axis_index("shard")
    mine = lax.axis_index("expert")
    per = final_gate.shape[0]
    rows, cols = gate.shape[1], gate.shape[2]
    sources, finals = (gate, up), (final_gate, final_up)

    order = sum_order(n)
    tables = [send_order(n, i) for i in range(n)]
    remote = [pick(me, [tables[i][k] for i in range(n)]) for k in range(n - 2)]
    partner = me + 1 - 2 * lax.rem(me, 2)
    targets = [remote[0], partner, me] + remote[1:]

    work = []
    for i in range(LEAD):
        work += [("sum", i, order[i], t) for t in (0, 1)]
    work += [("send", 0, targets[0], t) for t in (0, 1)]
    for i in range(LEAD, n):
        work += [("sum", i, order[i], t) for t in (0, 1)]
    for k in range(1, n):
        work += [("send", k, targets[k], t) for t in (0, 1)]

    def read(index):
        _, _, group, t = work[index]
        slot = index % SLOTS
        return pltpu.make_async_copy(
            sources[t].at[pl.ds(group * per, per)], ring.at[slot], read_sem.at[slot]
        )

    for index in range(SLOTS):
        read(index).start()

    def peer(j):
        return lax.rem(me + j, n)

    def other(j):
        return lax.rem(mine + j, ne)

    def psum_copy(group):
        return pltpu.make_async_remote_copy(
            src_ref=psum.at[group], dst_ref=parts.at[me], send_sem=psum_send.at[group],
            recv_sem=psum_recv.at[me], device_id={"shard": group}, device_id_type=MESH,
        )

    def psum_arrival(source):
        return pltpu.make_async_remote_copy(
            src_ref=parts.at[source], dst_ref=parts.at[source], send_sem=psum_send.at[source],
            recv_sem=psum_recv.at[source], device_id={"shard": source}, device_id_type=MESH,
        )

    def scale_copy(j):
        return pltpu.make_async_remote_copy(
            src_ref=scales.at[me], dst_ref=scales.at[me], send_sem=scale_send.at[j],
            recv_sem=scale_recv.at[me], device_id={"shard": peer(j)}, device_id_type=MESH,
        )

    def scale_arrival(group):
        return pltpu.make_async_remote_copy(
            src_ref=scales.at[group], dst_ref=scales.at[group], send_sem=scale_send.at[0],
            recv_sem=scale_recv.at[group], device_id={"shard": group}, device_id_type=MESH,
        )

    def kept(k):
        return k - (k > 2)

    def data_copy(k, t, e):
        return pltpu.make_async_remote_copy(
            src_ref=sbuf.at[kept(k), t * per + e],
            dst_ref=finals[t].at[e, pl.ds(me * rows, rows)],
            send_sem=data_send.at[k, t * per + e],
            recv_sem=data_recv.at[me, t * per + e],
            device_id={"shard": targets[k]}, device_id_type=MESH,
        )

    def data_arrival(source, t, e):
        return pltpu.make_async_remote_copy(
            src_ref=finals[t].at[e, pl.ds(source * rows, rows)],
            dst_ref=finals[t].at[e, pl.ds(source * rows, rows)],
            send_sem=data_send.at[0, t * per + e],
            recv_sem=data_recv.at[source, t * per + e],
            device_id={"shard": source}, device_id_type=MESH,
        )

    def row_copy(j):
        return pltpu.make_async_remote_copy(
            src_ref=routers.at[mine, me], dst_ref=routers.at[mine, me], send_sem=row_send.at[j],
            recv_sem=row_recv.at[me], device_id={"shard": peer(j)}, device_id_type=MESH,
        )

    def row_arrival(source):
        return pltpu.make_async_remote_copy(
            src_ref=routers.at[mine, source], dst_ref=routers.at[mine, source],
            send_sem=row_send.at[0], recv_sem=row_recv.at[source],
            device_id={"shard": source}, device_id_type=MESH,
        )

    def col_copy(j):
        return pltpu.make_async_remote_copy(
            src_ref=routers.at[mine], dst_ref=routers.at[mine], send_sem=col_send.at[j],
            recv_sem=col_recv.at[mine], device_id={"expert": other(j)}, device_id_type=MESH,
        )

    def col_arrival(source):
        return pltpu.make_async_remote_copy(
            src_ref=routers.at[source], dst_ref=routers.at[source], send_sem=col_send.at[0],
            recv_sem=col_recv.at[source], device_id={"expert": source}, device_id_type=MESH,
        )

    barrier = pltpu.get_barrier_semaphore()
    for j in range(1, n):
        pl.semaphore_signal(barrier, inc=1, device_id={"shard": peer(j)}, device_id_type=MESH)
    for j in range(1, ne):
        pl.semaphore_signal(barrier, inc=1, device_id={"expert": other(j)}, device_id_type=MESH)

    def sum_chunk(slot, group, t):
        def one(e, _):
            def block(b, total):
                start = pl.multiple_of(b * 8, 8)
                return total + jnp.abs(ring[slot, e, pl.ds(start, 8), :])

            total = lax.fori_loop(
                0, rows // 8, block, jnp.zeros((8, cols), jnp.float32), unroll=8
            )
            psum[group, pl.ds(t * per + e, 1), :] = jnp.sum(total, axis=0, keepdims=True)
            return 0

        lax.fori_loop(0, per, one, 0)

    def send_chunk(slot, k, group, t):
        def one(e, _):
            inverse = 1.0 / scales[group, pl.ds(t * per + e, 1), :]
            wide = jnp.broadcast_to(inverse, (16, cols))

            def block(b, _):
                start = pl.multiple_of(b * 16, 16)
                value = (ring[slot, e, pl.ds(start, 16), :] * wide).astype(jnp.bfloat16)
                if k == 2:
                    base = pl.multiple_of(me * rows + start, 16)
                    finals[t][e, pl.ds(base, 16), :] = value
                else:
                    sbuf[kept(k), t * per + e, pl.ds(start, 16), :] = value
                return 0

            lax.fori_loop(0, rows // 16, block, 0, unroll=4)
            if k != 2:
                data_copy(k, t, e).start()
            return 0

        lax.fori_loop(0, per, one, 0)

    def home():
        for j in range(1, n):
            psum_arrival(peer(j)).wait_recv()
        parts[me] = psum[me]
        total = parts[0]
        for i in range(1, n):
            total = total + parts[i]
        scale = total / rows_total
        scales[me] = scale
        for j in range(1, n):
            scale_copy(j).start()
        scale_gate[...] = scale[:per]
        scale_up[...] = scale[per:]

    early = me == order[0]
    for i in range(1, LEAD - 2):
        early = jnp.logical_or(early, me == order[i])

    for index, (kind, step, group, t) in enumerate(work):
        slot = index % SLOTS
        if kind == "sum" and t == 0 and step == LEAD - 1:
            pl.when(early)(home)
        if kind == "send" and t == 0:
            if step == 1:
                pl.when(jnp.logical_not(early))(home)
                routers[mine, me] = (router_t[...] * gain[...]).astype(jnp.bfloat16)
                for j in range(1, n):
                    row_copy(j).start()
            if step != 2:
                scale_arrival(group).wait_recv()
        read(index).wait()
        if kind == "sum":
            sum_chunk(slot, group, t)
            if t == 1:
                if step == 0:
                    pl.semaphore_wait(barrier, n - 1 + ne - 1)

                @pl.when(me != group)
                def _(group=group):
                    psum_copy(group).start()
        else:
            send_chunk(slot, step, group, t)
        if index + SLOTS < len(work):
            read(index + SLOTS).start()

    for j in range(1, n):
        row_arrival(peer(j)).wait_recv()
    for j in range(1, ne):
        col_copy(j).start()
    for j in range(1, ne):
        col_arrival(other(j)).wait_recv()
    wide, tall = routers.shape[2], routers.shape[3]
    for e in range(ne):
        for s in range(n):
            out_router_t[e * wide:(e + 1) * wide, s * tall:(s + 1) * tall] = routers[e, s]

    for j in range(1, n):
        psum_copy(peer(j)).wait_send()
        scale_copy(j).wait_send()
        row_copy(j).wait_send()
    for j in range(1, ne):
        col_copy(j).wait_send()
    for k in [k for k in range(n) if k != 2]:
        for t in (0, 1):

            def done(e, _, k=k, t=t):
                data_copy(k, t, e).wait_send()
                return 0

            lax.fori_loop(0, per, done, 0)
    for j in range(1, n):
        for t in (0, 1):

            def arrived(e, _, j=j, t=t):
                data_arrival(peer(j), t, e).wait_recv()
                return 0

            lax.fori_loop(0, per, arrived, 0)


def place(
    gate, up, scale_gate, scale_up, router_t,
    final_gate, final_up, out_gate, out_up, router, sems,
):
    copies = [
        pltpu.make_async_copy(gate, final_gate, sems.at[0]),
        pltpu.make_async_copy(up, final_up, sems.at[1]),
    ]
    for copy in copies:
        copy.start()
    out_gate[...] = scale_gate[...]
    out_up[...] = scale_up[...]
    router[...] = router_t[...].T
    for copy in copies:
        copy.wait()


def solution(mesh):
    n, ne = mesh.shape["shard"], mesh.shape["expert"]

    def body(master_gate, master_up, router_weight, router_gain):
        held, rows, cols = master_gate.shape
        per = held // n
        router_t = router_weight.T
        wide, tall = router_t.shape
        sem = pltpu.SemaphoreType.DMA
        vmem = pl.BlockSpec(memory_space=pltpu.VMEM)
        hbm = pl.BlockSpec(memory_space=pl.ANY)
        landed = pl.pallas_call(
            functools.partial(kernel, n, ne, rows * n),
            out_shape=(
                pltpu.VMEM((per, rows * n, cols), jnp.bfloat16),
                pltpu.VMEM((per, rows * n, cols), jnp.bfloat16),
                pltpu.VMEM((per, cols), jnp.float32),
                pltpu.VMEM((per, cols), jnp.float32),
                pltpu.VMEM((wide * ne, tall * n), jnp.bfloat16),
            ),
            in_specs=[
                pl.BlockSpec(memory_space=pl.ANY),
                pl.BlockSpec(memory_space=pl.ANY),
                pl.BlockSpec(memory_space=pltpu.VMEM),
                pl.BlockSpec(memory_space=pltpu.VMEM),
            ],
            out_specs=(vmem,) * 5,
            scratch_shapes=[
                pltpu.VMEM((SLOTS, per, rows, cols), jnp.float32),
                pltpu.VMEM((n - 1, 2 * per, rows, cols), jnp.bfloat16),
                pltpu.VMEM((n, 2 * per, cols), jnp.float32),
                pltpu.VMEM((n, 2 * per, cols), jnp.float32),
                pltpu.VMEM((n, 2 * per, cols), jnp.float32),
                pltpu.VMEM((ne, n, wide, tall), jnp.bfloat16),
                sem((SLOTS,)),
                sem((n,)), sem((n,)), sem((n,)), sem((n,)),
                sem((n, 2 * per)), sem((n, 2 * per)),
                sem((n,)), sem((n,)), sem((ne,)), sem((ne,)),
            ],
            compiler_params=pltpu.CompilerParams(
                collective_id=0, has_side_effects=True, vmem_limit_bytes=VMEM_BYTES
            ),
        )(master_gate, master_up, router_t, router_gain[None, :])
        return pl.pallas_call(
            place,
            out_shape=(
                jax.ShapeDtypeStruct((per, rows * n, cols), jnp.bfloat16),
                jax.ShapeDtypeStruct((per, rows * n, cols), jnp.bfloat16),
                jax.ShapeDtypeStruct((per, cols), jnp.float32),
                jax.ShapeDtypeStruct((per, cols), jnp.float32),
                jax.ShapeDtypeStruct((tall * n, wide * ne), jnp.bfloat16),
            ),
            in_specs=[vmem] * 5,
            out_specs=(hbm, hbm, vmem, vmem, vmem),
            scratch_shapes=[sem((2,))],
            compiler_params=pltpu.CompilerParams(vmem_limit_bytes=8 * 1024 * 1024),
        )(*landed)

    return jax.shard_map(
        body,
        mesh=mesh,
        in_specs=(
            P("expert", "shard", None),
            P("expert", "shard", None),
            P("shard", "expert"),
            P("shard"),
        ),
        out_specs=(
            P(("expert", "shard"), None, None),
            P(("expert", "shard"), None, None),
            P(("expert", "shard"), None),
            P(("expert", "shard"), None),
            P(),
        ),
        check_vma=False,
    )
```

```python
import functools

import jax
import jax.numpy as jnp
from jax import lax
from jax.experimental import pallas as pl
from jax.experimental.pallas import tpu as pltpu
from jax.sharding import PartitionSpec as P

MESH = pl.DeviceIdType.MESH
SLOTS = 4
LEAD = 4
VMEM_BYTES = 38 * 1024 * 1024


def sum_order(n):
    chips = n // 2
    return sorted(range(n), key=lambda g: (abs(2 * (g // 2) - (chips - 1)), g % 2, g))


def send_order(n, me):
    chip = me // 2
    order = sum_order(n)
    others = [g for g in range(n) if g // 2 != chip]
    near = sorted(others, key=lambda g: (abs(g // 2 - chip), g % 2, order.index(g)))
    first = next(g for g in near if g in order[:2])
    return [first] + [g for g in near if g != first]


def pick(me, values):
    result = jnp.int32(values[0])
    for i in range(1, len(values)):
        result = jnp.where(me == i, jnp.int32(values[i]), result)
    return result


def kernel(
    n, ne, rows_total,
    gate, up, router_t, gain,
    final_gate, final_up, scale_gate, scale_up, out_router_t,
    ring, sbuf, psum, parts, pairs, scales, routers,
    read_sem, psum_send, psum_recv, pair_recv, scale_send, scale_recv, pass_send,
    data_send, data_recv, row_send, row_recv, half_send, half_recv, col_send, col_recv,
):
    me = lax.axis_index("shard")
    mine = lax.axis_index("expert")
    per = final_gate.shape[0]
    rows, cols = gate.shape[1], gate.shape[2]
    sources, finals = (gate, up), (final_gate, final_up)

    order = sum_order(n)
    early, late = order[:2], order[2:]
    core, chip = lax.rem(me, 2), me // 2
    tables = [send_order(n, i) for i in range(n)]
    remote = [pick(me, [tables[i][k] for i in range(n)]) for k in range(n - 2)]
    partner = me + 1 - 2 * core
    targets = [remote[0], partner, me] + remote[1:]

    work = []
    for i in range(LEAD):
        work += [("sum", i, order[i], t) for t in (0, 1)]
    work += [("send", 0, targets[0], t) for t in (0, 1)]
    for i in range(LEAD, n):
        work += [("sum", i, order[i], t) for t in (0, 1)]
    for k in range(1, n):
        work += [("send", k, targets[k], t) for t in (0, 1)]

    def read(index):
        _, _, group, t = work[index]
        slot = index % SLOTS
        return pltpu.make_async_copy(
            sources[t].at[pl.ds(group * per, per)], ring.at[slot], read_sem.at[slot]
        )

    for index in range(SLOTS):
        read(index).start()

    def peer(j):
        return lax.rem(me + j, n)

    def other(j):
        return lax.rem(mine + j, ne)

    def psum_copy(group):
        return pltpu.make_async_remote_copy(
            src_ref=psum.at[group], dst_ref=parts.at[me], send_sem=psum_send.at[group],
            recv_sem=psum_recv.at[me], device_id={"shard": group}, device_id_type=MESH,
        )

    def pair_copy(group):
        return pltpu.make_async_remote_copy(
            src_ref=psum.at[group], dst_ref=pairs.at[group], send_sem=psum_send.at[group],
            recv_sem=pair_recv.at[group], device_id={"shard": partner}, device_id_type=MESH,
        )

    def psum_arrival(source):
        return pltpu.make_async_remote_copy(
            src_ref=parts.at[source], dst_ref=parts.at[source], send_sem=psum_send.at[source],
            recv_sem=psum_recv.at[source], device_id={"shard": source}, device_id_type=MESH,
        )

    def scale_copy(j, target):
        return pltpu.make_async_remote_copy(
            src_ref=scales.at[me], dst_ref=scales.at[me], send_sem=scale_send.at[j],
            recv_sem=scale_recv.at[me], device_id={"shard": target}, device_id_type=MESH,
        )

    def scale_pass(group):
        return pltpu.make_async_remote_copy(
            src_ref=scales.at[group], dst_ref=scales.at[group], send_sem=pass_send.at[group],
            recv_sem=scale_recv.at[group], device_id={"shard": partner}, device_id_type=MESH,
        )

    def scale_arrival(group):
        return pltpu.make_async_remote_copy(
            src_ref=scales.at[group], dst_ref=scales.at[group], send_sem=scale_send.at[0],
            recv_sem=scale_recv.at[group], device_id={"shard": group}, device_id_type=MESH,
        )

    def kept(k):
        return k - (k > 2)

    def data_copy(k, t, e):
        return pltpu.make_async_remote_copy(
            src_ref=sbuf.at[kept(k), t * per + e],
            dst_ref=finals[t].at[e, pl.ds(me * rows, rows)],
            send_sem=data_send.at[k, t * per + e],
            recv_sem=data_recv.at[me, t * per + e],
            device_id={"shard": targets[k]}, device_id_type=MESH,
        )

    def data_arrival(source, t, e):
        return pltpu.make_async_remote_copy(
            src_ref=finals[t].at[e, pl.ds(source * rows, rows)],
            dst_ref=finals[t].at[e, pl.ds(source * rows, rows)],
            send_sem=data_send.at[0, t * per + e],
            recv_sem=data_recv.at[source, t * per + e],
            device_id={"shard": source}, device_id_type=MESH,
        )

    def row_copy(j):
        return pltpu.make_async_remote_copy(
            src_ref=routers.at[mine, core, chip], dst_ref=routers.at[mine, core, chip],
            send_sem=row_send.at[j], recv_sem=row_recv.at[chip],
            device_id={"shard": peer(j)}, device_id_type=MESH,
        )

    def row_arrival(j):
        source = peer(j)
        return pltpu.make_async_remote_copy(
            src_ref=routers.at[mine, core, source // 2], dst_ref=routers.at[mine, core, source // 2],
            send_sem=row_send.at[j], recv_sem=row_recv.at[source // 2],
            device_id={"shard": source}, device_id_type=MESH,
        )

    def half_copy(half):
        return pltpu.make_async_remote_copy(
            src_ref=routers.at[mine, half], dst_ref=routers.at[mine, half],
            send_sem=half_send.at[0], recv_sem=half_recv.at[0],
            device_id={"shard": partner}, device_id_type=MESH,
        )

    def col_copy(j):
        return pltpu.make_async_remote_copy(
            src_ref=routers.at[mine], dst_ref=routers.at[mine], send_sem=col_send.at[j],
            recv_sem=col_recv.at[mine], device_id={"expert": other(j)}, device_id_type=MESH,
        )

    def col_arrival(source):
        return pltpu.make_async_remote_copy(
            src_ref=routers.at[source], dst_ref=routers.at[source], send_sem=col_send.at[0],
            recv_sem=col_recv.at[source], device_id={"expert": source}, device_id_type=MESH,
        )

    barrier = pltpu.get_barrier_semaphore()
    for j in range(1, n):
        pl.semaphore_signal(barrier, inc=1, device_id={"shard": peer(j)}, device_id_type=MESH)
    for j in range(1, ne):
        pl.semaphore_signal(barrier, inc=1, device_id={"expert": other(j)}, device_id_type=MESH)

    def sum_chunk(slot, group, t):
        def one(e, _):
            def block(b, total):
                start = pl.multiple_of(b * 8, 8)
                return total + jnp.abs(ring[slot, e, pl.ds(start, 8), :])

            total = lax.fori_loop(
                0, rows // 8, block, jnp.zeros((8, cols), jnp.float32), unroll=8
            )
            psum[group, pl.ds(t * per + e, 1), :] = jnp.sum(total, axis=0, keepdims=True)
            return 0

        lax.fori_loop(0, per, one, 0)

    def send_chunk(slot, k, group, t):
        def one(e, _):
            inverse = 1.0 / scales[group, pl.ds(t * per + e, 1), :]
            wide = jnp.broadcast_to(inverse, (16, cols))

            def block(b, _):
                start = pl.multiple_of(b * 16, 16)
                value = (ring[slot, e, pl.ds(start, 16), :] * wide).astype(jnp.bfloat16)
                if k == 2:
                    base = pl.multiple_of(me * rows + start, 16)
                    finals[t][e, pl.ds(base, 16), :] = value
                else:
                    sbuf[kept(k), t * per + e, pl.ds(start, 16), :] = value
                return 0

            lax.fori_loop(0, rows // 16, block, 0, unroll=4)
            if k != 2:
                data_copy(k, t, e).start()
            return 0

        lax.fori_loop(0, per, one, 0)

    def finish(sources):
        total = psum[me]
        for source in sources:
            psum_arrival(source).wait_recv()
            total = total + parts[source]
        scale = total / rows_total
        scales[me] = scale
        scale_gate[...] = scale[:per]
        scale_up[...] = scale[per:]

    def home_early():
        finish([peer(j) for j in range(1, n)])
        for j in range(1, n):
            scale_copy(j, peer(j)).start()

    def home_late():
        finish([peer(j) for j in range(2, n, 2)])
        scale_copy(1, partner).start()
        for j in range(2, n, 2):
            scale_copy(j, peer(j)).start()

    def combine(group):
        pair_copy(group).wait_recv()
        psum[group] = psum[group] + pairs[group]

        @pl.when(me != group)
        def _():
            psum_copy(group).start()

    is_early = jnp.logical_or(me == early[0], me == early[1])

    def exchange_late():
        for group in late:
            pl.when(core == group % 2)(functools.partial(combine, group))
        pl.when(jnp.logical_not(is_early))(home_late)
        for group in late:

            @pl.when(jnp.logical_and(core == group % 2, me != group))
            def _(group=group):
                scale_arrival(group).wait_recv()
                scale_pass(group).start()

        for group in late:

            @pl.when(core != group % 2)
            def _(group=group):
                scale_arrival(group).wait_recv()

        for group in early:

            @pl.when(jnp.logical_and(me != group, targets[0] != group))
            def _(group=group):
                scale_arrival(group).wait_recv()

    for index, (kind, step, group, t) in enumerate(work):
        slot = index % SLOTS
        if kind == "sum" and t == 0 and step == LEAD - 1:
            pl.when(is_early)(home_early)
        if kind == "send" and t == 0:
            if step == 0:
                scale_arrival(group).wait_recv()
            elif step == 1:
                exchange_late()
                routers[mine, core, chip] = (router_t[...] * gain[...]).astype(jnp.bfloat16)
                for j in range(2, n, 2):
                    row_copy(j).start()
        read(index).wait()
        if kind == "sum":
            sum_chunk(slot, group, t)
            if t == 1:
                if step == 0:
                    pl.semaphore_wait(barrier, n - 1 + ne - 1)

                if group in early:

                    @pl.when(me != group)
                    def _(group=group):
                        psum_copy(group).start()
                else:

                    @pl.when(core != group % 2)
                    def _(group=group):
                        pair_copy(group).start()
        else:
            send_chunk(slot, step, group, t)
        if index + SLOTS < len(work):
            read(index + SLOTS).start()

    for j in range(2, n, 2):
        row_arrival(j).wait_recv()
    half_copy(core).start()
    half_copy(1 - core).wait_recv()
    for j in range(1, ne):
        col_copy(j).start()
    for j in range(1, ne):
        col_arrival(other(j)).wait_recv()
    wide, tall = routers.shape[3], routers.shape[4]
    for e in range(ne):
        for s in range(n):
            out_router_t[e * wide:(e + 1) * wide, s * tall:(s + 1) * tall] = routers[e, s % 2, s // 2]

    for j in range(1, n):
        psum_copy(peer(j)).wait_send()
    scale_copy(1, partner).wait_send()
    for j in range(2, n, 2):
        scale_copy(j, peer(j)).wait_send()
        row_copy(j).wait_send()

    @pl.when(is_early)
    def _():
        for j in range(3, n, 2):
            scale_copy(j, peer(j)).wait_send()

    for group in late:

        @pl.when(jnp.logical_and(core == group % 2, me != group))
        def _(group=group):
            scale_pass(group).wait_send()

    half_copy(core).wait_send()
    for j in range(1, ne):
        col_copy(j).wait_send()
    for k in [k for k in range(n) if k != 2]:
        for t in (0, 1):

            def done(e, _, k=k, t=t):
                data_copy(k, t, e).wait_send()
                return 0

            lax.fori_loop(0, per, done, 0)
    for j in range(1, n):
        for t in (0, 1):

            def arrived(e, _, j=j, t=t):
                data_arrival(peer(j), t, e).wait_recv()
                return 0

            lax.fori_loop(0, per, arrived, 0)


def place(
    gate, up, scale_gate, scale_up, router_t,
    final_gate, final_up, out_gate, out_up, router, turned, sems, small,
):
    copies = []
    for e in range(gate.shape[0]):
        copies.append(pltpu.make_async_copy(gate.at[e], final_gate.at[e], sems.at[0, e]))
        copies.append(pltpu.make_async_copy(up.at[e], final_up.at[e], sems.at[1, e]))
    copies.append(pltpu.make_async_copy(scale_gate, out_gate, small.at[0]))
    copies.append(pltpu.make_async_copy(scale_up, out_up, small.at[1]))
    for copy in copies:
        copy.start()
    turned[...] = router_t[...].T
    last = pltpu.make_async_copy(turned, router, small.at[2])
    last.start()
    for copy in copies + [last]:
        copy.wait()


def solution(mesh):
    n, ne = mesh.shape["shard"], mesh.shape["expert"]

    def body(master_gate, master_up, router_weight, router_gain):
        held, rows, cols = master_gate.shape
        per = held // n
        router_t = router_weight.T
        wide, tall = router_t.shape
        sem = pltpu.SemaphoreType.DMA
        vmem = pl.BlockSpec(memory_space=pltpu.VMEM)
        hbm = pl.BlockSpec(memory_space=pl.ANY)
        landed = pl.pallas_call(
            functools.partial(kernel, n, ne, rows * n),
            out_shape=(
                pltpu.VMEM((per, rows * n, cols), jnp.bfloat16),
                pltpu.VMEM((per, rows * n, cols), jnp.bfloat16),
                pltpu.VMEM((per, cols), jnp.float32),
                pltpu.VMEM((per, cols), jnp.float32),
                pltpu.VMEM((wide * ne, tall * n), jnp.bfloat16),
            ),
            in_specs=[
                pl.BlockSpec(memory_space=pl.ANY),
                pl.BlockSpec(memory_space=pl.ANY),
                pl.BlockSpec(memory_space=pltpu.VMEM),
                pl.BlockSpec(memory_space=pltpu.VMEM),
            ],
            out_specs=(vmem,) * 5,
            scratch_shapes=[
                pltpu.VMEM((SLOTS, per, rows, cols), jnp.float32),
                pltpu.VMEM((n - 1, 2 * per, rows, cols), jnp.bfloat16),
                pltpu.VMEM((n, 2 * per, cols), jnp.float32),
                pltpu.VMEM((n, 2 * per, cols), jnp.float32),
                pltpu.VMEM((n, 2 * per, cols), jnp.float32),
                pltpu.VMEM((n, 2 * per, cols), jnp.float32),
                pltpu.VMEM((ne, 2, n // 2, wide, tall), jnp.bfloat16),
                sem((SLOTS,)),
                sem((n,)), sem((n,)), sem((n,)), sem((n,)), sem((n,)), sem((n,)),
                sem((n, 2 * per)), sem((n, 2 * per)),
                sem((n,)), sem((n // 2,)), sem((1,)), sem((1,)), sem((ne,)), sem((ne,)),
            ],
            compiler_params=pltpu.CompilerParams(
                collective_id=0, has_side_effects=True, vmem_limit_bytes=VMEM_BYTES
            ),
        )(master_gate, master_up, router_t, router_gain[None, :])
        return pl.pallas_call(
            place,
            out_shape=(
                jax.ShapeDtypeStruct((per, rows * n, cols), jnp.bfloat16),
                jax.ShapeDtypeStruct((per, rows * n, cols), jnp.bfloat16),
                jax.ShapeDtypeStruct((per, cols), jnp.float32),
                jax.ShapeDtypeStruct((per, cols), jnp.float32),
                jax.ShapeDtypeStruct((tall * n, wide * ne), jnp.bfloat16),
            ),
            in_specs=[vmem] * 5,
            out_specs=(hbm,) * 5,
            scratch_shapes=[
                pltpu.VMEM((tall * n, wide * ne), jnp.bfloat16), sem((2, per)), sem((3,)),
            ],
            compiler_params=pltpu.CompilerParams(vmem_limit_bytes=8 * 1024 * 1024),
        )(*landed)

    return jax.shard_map(
        body,
        mesh=mesh,
        in_specs=(
            P("expert", "shard", None),
            P("expert", "shard", None),
            P("shard", "expert"),
            P("shard"),
        ),
        out_specs=(
            P(("expert", "shard"), None, None),
            P(("expert", "shard"), None, None),
            P(("expert", "shard"), None),
            P(("expert", "shard"), None),
            P(),
        ),
        check_vma=False,
    )
```
